32 devices in a mesh: grp: 2 (over x), shard: 16 (over z, y, core).
Axes of the slice: x: 2, y: 2, z: 4, core: 2. Of those that a mesh axis runs over, the one named last changes fastest.
Arguments:
- window: bfloat16 [32, 4096], P('grp'), may hold values from -6 to 6
- weight: bfloat16 [11008, 4096], P('shard'), may hold values from -0.09375 to 0.09375
- factor_a: bfloat16 [64, 4, 4096], P(('grp', 'shard')), may hold values from -6 to 6
- factor_b: bfloat16 [64, 4, 11008], P(('grp', 'shard')), may hold values from -6 to 6
- fitness: float32 [64], P(('grp', 'shard')), may hold values from -4 to 4
Outputs:
- perturbed: bfloat16 [11008, 1024], P('shard', 'grp')
- update: float32 [11008, 4096], P('shard', 'grp')
The draws below stay inside these ranges and needn't reach their ends.
All inputs are finite; a program needn't handle non-finite values.
Results may differ from the reference program's by a relative error of at most 0.0029.
Values may be sent and summed in bfloat16 or wider, within the bound.
A program may use at most 64 MiB of HBM per device.

```python
import math
import jax
import jax.numpy as jnp
from jax import lax

D = 4096
FF = 11008
TOK = 16
RANK = 4
CANDS = 64
N_GRP = 2


def levels(rng, extent, split, smallest, high):
    def one(dim, blocks):
        draws = jax.random.uniform(jax.random.fold_in(jax.random.fold_in(rng, 6), dim), (blocks,), jnp.float32, smallest / len(split), high / len(split))
        return jnp.repeat(jnp.exp(draws), extent[dim] // blocks).reshape((-1,) + (1,) * (len(extent) - dim - 1))

    level = one(*split[0])
    for cut in split[1:]:
        level = level * one(*cut)
    return level


def normal_values(own_key, shape, width, most, pieces=(), kind=jnp.bfloat16):
    gain = levels(own_key, shape, pieces, -0.22, 0.18) if pieces else 1.0
    values = jax.random.normal(own_key, shape, jnp.float32) * width * gain
    return jnp.minimum(jnp.maximum(values, -most), most).astype(kind)


def setup_inputs(seed: int = 0) -> dict:
    streams_of = jax.random.split(jax.random.key(seed), 6)
    window = normal_values(streams_of[0], (N_GRP * TOK, D), 1.0, 6.0, ((0, 2),))
    weight = normal_values(streams_of[1], (FF, D), D ** -0.5, 0.09375, ((0, 16),))
    factor_a = normal_values(streams_of[2], (CANDS, RANK, D), 1.0, 6.0, ((0, 32),))
    factor_b = normal_values(streams_of[3], (CANDS, RANK, FF), 1.0, 6.0, ((0, 32),))
    fitness = normal_values(streams_of[4], (CANDS,), 1.0, 4.0, ((0, 32),), jnp.float32)
    return {"window": window, "weight": weight, "factor_a": factor_a, "factor_b": factor_b, "fitness": fitness}


def reference(window, weight, factor_a, factor_b, fitness):
    total_cands = factor_a.shape[0]
    group_count = window.shape[0] // TOK
    per_group = total_cands // group_count
    perturb = 0.25 / math.sqrt(D)
    base_out = jnp.dot(window, weight.T, preferred_element_type=jnp.float32).reshape(group_count, TOK, FF)
    x_groups = window.reshape(group_count, TOK, D)
    a_groups = factor_a.reshape(group_count, per_group, RANK, D)
    b_groups = factor_b.reshape(group_count, per_group, RANK, FF)

    def one_group(inputs):
        group_window, group_a, group_b, group_base = inputs
        projected = jnp.einsum('td,crd->crt', group_window.astype(jnp.float32), group_a.astype(jnp.float32), precision=lax.Precision.HIGHEST)
        low_rank = jnp.einsum('crt,crf->ctf', projected, group_b.astype(jnp.float32), precision=lax.Precision.HIGHEST)
        return (group_base[None] + perturb * low_rank).astype(jnp.bfloat16)
    perturbed = lax.map(one_group, (x_groups, a_groups, b_groups, base_out)).reshape(total_cands * TOK, FF).T
    weighted = (fitness[:, None, None] * factor_b.astype(jnp.float32)).astype(jnp.bfloat16)
    update = jnp.dot(weighted.reshape(total_cands * RANK, FF).T, factor_a.reshape(total_cands * RANK, D), preferred_element_type=jnp.float32)
    update = update * (0.5 / math.sqrt(total_cands))
    return (perturbed, update)
```

```python
import functools
import math

import jax
import jax.numpy as jnp
from jax import lax
from jax.experimental import pallas as pl
from jax.experimental.pallas import tpu as pltpu
from jax.sharding import PartitionSpec as P

MESH = pl.DeviceIdType.MESH
F32 = jnp.float32
BF16 = jnp.bfloat16
ROW_CHUNK = 128


def dot_rows(left, right):
    return lax.dot_general(left, right, (((1,), (1,)), ((), ())), preferred_element_type=F32)


def dot_cols(left, right):
    return lax.dot_general(left, right, (((0,), (0,)), ((), ())), preferred_element_type=F32)


def exchange_kernel(
    n_grp, n_shard, fit_ref, win_ref, a_ref, b_ref, weight_ref,
    a_all, b_all, small_all, base_ref,
    small, weight, w_sem, b_send, b_recv, s_send, s_recv,
    a_send, a_send2, a_send3, a_recv1, a_recv2, a_recv3,
):
    depth = n_shard // 4
    count = n_grp * n_shard
    line = n_grp * depth
    grp = lax.axis_index("grp")
    shard = lax.axis_index("shard")
    core = shard % 2
    y = (shard // 2) % 2
    z = shard // 4
    me = grp * n_shard + shard
    own = core * (2 * line) + y * line + grp * depth + z
    half = a_all.shape[2]
    rows = b_ref.shape[1]
    ff = weight_ref.shape[0]
    cand_dev = fit_ref.shape[0]
    rank = rows // cand_dev
    tok = win_ref.shape[0]

    chunks = [(lo, min(ROW_CHUNK, ff - lo)) for lo in range(0, ff, ROW_CHUNK)]
    loads = [
        pltpu.make_async_copy(
            weight_ref.at[pl.ds(lo, size)], weight.at[pl.ds(lo, size)], w_sem.at[i]
        )
        for i, (lo, size) in enumerate(chunks)
    ]
    for load in loads:
        load.start()

    barrier = pltpu.get_barrier_semaphore()

    def greet(i, carry):
        t = (me + i) % count
        pl.semaphore_signal(
            barrier, inc=1, device_id=(t // n_shard, t % n_shard), device_id_type=MESH
        )
        return carry

    lax.fori_loop(1, count, greet, 0)
    pl.semaphore_wait(barrier, count - 1)

    def place(i):
        return (grp + i // depth) % n_grp, (z + i) % depth

    def origin(i):
        return (grp + n_grp - i // depth) % n_grp, (z + depth - i % depth) % depth

    def a_source(g):
        return a_ref.at[:, pl.ds(pl.multiple_of(g * half, half), half)]

    def send_a(i, carry):
        g, zz = place(i)
        pltpu.make_async_remote_copy(
            src_ref=a_source(g),
            dst_ref=a_all.at[own],
            send_sem=a_send,
            recv_sem=a_recv1.at[i],
            device_id=(g, zz * 4 + y * 2 + core),
            device_id_type=MESH,
        ).start()
        return carry

    lax.fori_loop(1, line, send_a, 0)
    pltpu.make_async_copy(a_source(grp), a_all.at[own], a_recv1.at[0]).start()

    def send_b(i, carry):
        t = (me + i) % count
        pltpu.make_async_remote_copy(
            src_ref=b_ref.at[t % n_shard],
            dst_ref=b_all.at[own],
            send_sem=b_send,
            recv_sem=b_recv,
            device_id=(t // n_shard, t % n_shard),
            device_id_type=MESH,
        ).start()
        return carry

    lax.fori_loop(1, count, send_b, 0)
    pltpu.make_async_copy(b_ref.at[shard], b_all.at[own], b_recv).start()

    win = win_ref[...]
    projected = dot_rows(a_ref[...], win)
    row = lax.broadcasted_iota(jnp.int32, (rows, tok), 0)
    fit = jnp.zeros((rows, tok), F32)
    for j in range(cand_dev):
        fit = jnp.where(row // rank == j, fit_ref[j], fit)
    small[...] = jnp.zeros(small.shape, F32)
    small[:, :tok] = projected
    small[:, tok : 2 * tok] = fit

    def forward_y(i):
        g, zz = origin(i)
        slot = core * (2 * line) + y * line + g * depth + zz
        return pltpu.make_async_remote_copy(
            src_ref=a_all.at[slot],
            dst_ref=a_all.at[slot],
            send_sem=a_send2,
            recv_sem=a_recv2.at[i],
            device_id=(grp, z * 4 + (1 - y) * 2 + core),
            device_id_type=MESH,
        )

    def forward_core(i, yy):
        g, zz = origin(i)
        slot = core * (2 * line) + yy * line + g * depth + zz
        return pltpu.make_async_remote_copy(
            src_ref=a_all.at[slot],
            dst_ref=a_all.at[slot],
            send_sem=a_send3,
            recv_sem=a_recv3,
            device_id=(grp, z * 4 + y * 2 + (1 - core)),
            device_id_type=MESH,
        )

    def relay(i, carry):
        pltpu.make_async_copy(a_all.at[0], a_all.at[0], a_recv1.at[i]).wait()
        forward_y(i).start()
        forward_core(i, y).start()
        return carry

    def base_chunk(i):
        lo, size = chunks[i]
        loads[i].wait()
        win3 = jnp.concatenate([win, win, win], axis=0)
        base = dot_rows(weight[pl.ds(lo, size)], win3)
        high = base.astype(BF16)
        rest = base - high.astype(F32)
        mid = rest.astype(BF16)
        low = (rest - mid.astype(F32)).astype(BF16)
        part = lax.broadcasted_iota(jnp.int32, base.shape, 1) // tok
        terms = jnp.where(
            part == 0, high.astype(F32), jnp.where(part == 1, mid.astype(F32), low.astype(F32))
        )
        base_ref[pl.ds(lo, size), :] = terms.astype(BF16)

    lax.fori_loop(0, 1, relay, 0)
    base_chunk(0)

    def send_small(i, carry):
        t = (me + i) % count
        pltpu.make_async_remote_copy(
            src_ref=small,
            dst_ref=small_all.at[own],
            send_sem=s_send,
            recv_sem=s_recv,
            device_id=(t // n_shard, t % n_shard),
            device_id_type=MESH,
        ).start()
        return carry

    lax.fori_loop(1, count, send_small, 0)
    pltpu.make_async_copy(small, small_all.at[own], s_recv).start()
    for i in range(1, len(chunks)):
        base_chunk(i)

    lax.fori_loop(1, line, relay, 0)

    def relay2(i, carry):
        pltpu.make_async_copy(a_all.at[0], a_all.at[0], a_recv2.at[i]).wait()
        forward_core(i, 1 - y).start()
        return carry

    lax.fori_loop(0, line, relay2, 0)

    def wait_bytes(ref, sem):
        pltpu.make_async_copy(ref, ref, sem).wait()

    wait_bytes(small_all, s_recv)
    wait_bytes(b_all, b_recv)
    wait_bytes(a_all.at[pl.ds(0, 2 * line)], a_recv3)
    wait_bytes(a_all.at[pl.ds(0, line - 1)], a_send)
    wait_bytes(a_all.at[pl.ds(0, line)], a_send2)
    wait_bytes(a_all.at[pl.ds(0, 2 * line)], a_send3)
    wait_bytes(b_all.at[pl.ds(0, count - 1)], b_send)
    wait_bytes(small_all.at[pl.ds(0, count - 1)], s_send)


def combine_kernel(
    n_grp, n_shard, tok, rank, perturb, step_scale,
    a_ref, b_ref, small_ref, base_ref, pert_ref, upd_ref, weighted,
):
    depth = n_shard // 4
    count, rows, ff = b_ref.shape
    step = pl.program_id(0)
    cand_dev = rows // rank

    @pl.when(step == 0)
    def _():
        fit = small_ref[...][:, :, tok : tok + 1]
        scaled = fit * b_ref[...].astype(F32)
        weighted[...] = scaled.reshape(count * rows, ff).astype(BF16)

    width = upd_ref.shape[1]
    at = pl.ds(pl.multiple_of(step * width, width), width)
    block = a_ref[:, :, at].astype(F32).reshape(count * rows, width).astype(BF16)
    upd_ref[...] = dot_cols(weighted[...], block) * step_scale

    @pl.when(step == 0)
    def _():
        grp = lax.axis_index("grp")
        cols = pert_ref.shape[1]
        picks = [pl.ds(cy * n_grp * depth + grp * depth, depth) for cy in range(4)]
        own_b = jnp.concatenate([b_ref[p].astype(F32) for p in picks], axis=0)
        own_p = jnp.concatenate([small_ref[p] for p in picks], axis=0)
        k = n_shard * rows
        own_b = own_b.reshape(k, ff).astype(BF16)
        own_p = own_p.reshape(k, own_p.shape[2])[:, :tok] * perturb
        high = own_p.astype(BF16)
        low = (own_p - high.astype(F32)).astype(BF16)
        spread = (
            lax.broadcasted_iota(jnp.int32, (tok, cols), 1) % tok
            == lax.broadcasted_iota(jnp.int32, (tok, cols), 0)
        ).astype(F32).astype(BF16)
        r = lax.broadcasted_iota(jnp.int32, (k, cols), 0)
        slab = r // rows
        cy = slab // depth
        sh = (slab % depth) * 4 + (cy % 2) * 2 + cy // 2
        cand = sh * cand_dev + (r % rows) // rank
        keep = cand == lax.broadcasted_iota(jnp.int32, (k, cols), 1) // tok
        wide = lambda v: jnp.where(
            keep, jnp.dot(v, spread, preferred_element_type=F32), 0.0
        ).astype(BF16)
        spread3 = jnp.concatenate([spread, spread, spread], axis=0)
        total = jnp.dot(base_ref[...], spread3, preferred_element_type=F32)
        total = total + dot_cols(own_b, wide(high)) + dot_cols(own_b, wide(low))
        pert_ref[...] = total.astype(BF16)


def local(window, weight, factor_a, factor_b, fitness):
    tok, model_width = window.shape
    cand_dev, rank, _ = factor_a.shape
    n_shard = lax.axis_size("shard")
    n_grp = lax.axis_size("grp")
    total_cands = cand_dev * n_grp * n_shard
    perturb = 0.25 / math.sqrt(model_width)
    step_scale = 0.5 / math.sqrt(total_cands)
    rows = cand_dev * rank
    ff = weight.shape[0]
    half = model_width // n_grp
    count = n_grp * n_shard
    line = n_grp * (n_shard // 4)
    a_rows = factor_a.reshape(rows, model_width)
    b_slabs = factor_b.reshape(rows, n_shard, ff).transpose(1, 0, 2)

    n_chunks = -(-ff // ROW_CHUNK)
    vmem = pl.BlockSpec(memory_space=pltpu.VMEM)
    dma = pltpu.SemaphoreType.DMA
    a_all, b_all, small_all, base = pl.pallas_call(
        functools.partial(exchange_kernel, n_grp, n_shard),
        out_shape=(
            jax.ShapeDtypeStruct((count, rows, half), BF16),
            jax.ShapeDtypeStruct((count, rows, ff), BF16),
            jax.ShapeDtypeStruct((count, rows, 128), F32),
            jax.ShapeDtypeStruct((ff, 3 * tok), BF16),
        ),
        in_specs=[
            pl.BlockSpec(memory_space=pltpu.SMEM), vmem, vmem, vmem,
            pl.BlockSpec(memory_space=pl.ANY),
        ],
        out_specs=(vmem, vmem, vmem, vmem),
        scratch_shapes=[
            pltpu.VMEM((rows, 128), F32),
            pltpu.VMEM((ff, model_width), BF16),
            dma((n_chunks,)),
            dma, dma, dma, dma, dma, dma, dma,
            dma((line,)), dma((line,)), dma,
        ],
        compiler_params=pltpu.CompilerParams(
            collective_id=0, has_side_effects=True, vmem_limit_bytes=60 * 1024 * 1024
        ),
        name="exchange",
    )(fitness, window, a_rows, b_slabs, weight)

    block = min(half, 512)
    cols = n_shard * cand_dev * tok
    whole = lambda shape: pl.BlockSpec(shape, lambda i: (0,) * len(shape))
    perturbed, update = pl.pallas_call(
        functools.partial(combine_kernel, n_grp, n_shard, tok, rank, perturb, step_scale),
        out_shape=(
            jax.ShapeDtypeStruct((ff, cols), BF16),
            jax.ShapeDtypeStruct((ff, half), F32),
        ),
        grid=(half // block,),
        in_specs=[
            vmem, vmem, vmem, vmem,
        ],
        out_specs=(
            whole((ff, cols)),
            pl.BlockSpec((ff, block), lambda i: (0, i)),
        ),
        scratch_shapes=[pltpu.VMEM((count * rows, ff), BF16)],
        compiler_params=pltpu.CompilerParams(vmem_limit_bytes=56 * 1024 * 1024),
        name="combine",
    )(a_all, b_all, small_all, base)
    return perturbed, update


def solution(mesh):
    in_specs = (
        P("grp", None),
        P("shard", None),
        P(("grp", "shard"), None, None),
        P(("grp", "shard"), None, None),
        P(("grp", "shard")),
    )
    out_specs = (P("shard", "grp"), P("shard", "grp"))
    return jax.shard_map(local, mesh=mesh, in_specs=in_specs, out_specs=out_specs, check_vma=False)
```

```python
import functools
import math

import jax
import jax.numpy as jnp
from jax import lax
from jax.experimental import pallas as pl
from jax.experimental.pallas import tpu as pltpu
from jax.sharding import PartitionSpec as P

MESH = pl.DeviceIdType.MESH
F32 = jnp.float32
BF16 = jnp.bfloat16
ROW_CHUNK = 128


def dot_rows(left, right):
    return lax.dot_general(left, right, (((1,), (1,)), ((), ())), preferred_element_type=F32)


def dot_cols(left, right):
    return lax.dot_general(left, right, (((0,), (0,)), ((), ())), preferred_element_type=F32)


def exchange_kernel(
    n_grp, n_shard, fit_hbm, win_hbm, a_hbm, b_hbm, weight_ref,
    a_all, b_all, small_all, base_ref,
    fit_ref, win_ref, a_ref, b_ref, in_sem,
    a_rows, b_slabs, small, weight, w_sem, b_send, b_recv, s_send, s_recv,
    a_send, a_send_z, a_send_y, a_send_c, a_recv, a_recv_z, a_recv_y, a_recv_c,
):
    depth = n_shard // 8
    count = n_grp * n_shard
    line = n_grp * depth
    grp = lax.axis_index("grp")
    shard = lax.axis_index("shard")
    core = shard % 2
    y = (shard // 2) % 2
    low_z = (shard // 4) % 2
    high_z = shard // 8
    me = grp * n_shard + shard
    half = a_all.shape[2]
    cand_dev, rank, _ = a_ref.shape
    rows = cand_dev * rank
    ff = weight_ref.shape[0]
    tok = win_ref.shape[0]

    def slot_of(c, yy, lz, i):
        return ((c * 2 + yy) * 2 + lz) * line + i

    own = slot_of(core, y, low_z, grp * depth + high_z)

    inputs = [
        pltpu.make_async_copy(src, dst, in_sem.at[i])
        for i, (src, dst) in enumerate(
            [(a_hbm, a_ref), (b_hbm, b_ref), (win_hbm, win_ref), (fit_hbm, fit_ref)]
        )
    ]
    for load in inputs:
        load.start()

    barrier = pltpu.get_barrier_semaphore()

    def greet(i, carry):
        t = (me + i) % count
        pl.semaphore_signal(
            barrier, inc=1, device_id=(t // n_shard, t % n_shard), device_id_type=MESH
        )
        return carry

    lax.fori_loop(1, count, greet, 0)

    chunks = [(lo, min(ROW_CHUNK, ff - lo)) for lo in range(0, ff, ROW_CHUNK)]
    loads = [
        pltpu.make_async_copy(
            weight_ref.at[pl.ds(lo, size)], weight.at[pl.ds(lo, size)], w_sem.at[i]
        )
        for i, (lo, size) in enumerate(chunks)
    ]
    for load in loads:
        load.start()

    inputs[0].wait()
    a_rows[...] = jnp.concatenate(
        [a_ref[j].astype(F32) for j in range(cand_dev)], axis=0
    ).astype(BF16)
    inputs[1].wait()
    for k in range(n_shard):
        b_slabs[k] = jnp.concatenate(
            [b_ref[j, :, k * ff : (k + 1) * ff].astype(F32) for j in range(cand_dev)], axis=0
        ).astype(BF16)

    pl.semaphore_wait(barrier, count - 1)

    def origin(i):
        g = (grp + n_grp - i // depth) % n_grp
        return g * depth + (high_z + depth - i % depth) % depth

    def a_source(g):
        return a_rows.at[:, pl.ds(pl.multiple_of(g * half, half), half)]

    def send_a(i, carry):
        g = (grp + i // depth) % n_grp
        h = (high_z + i) % depth
        pltpu.make_async_remote_copy(
            src_ref=a_source(g),
            dst_ref=a_all.at[own],
            send_sem=a_send,
            recv_sem=a_recv.at[i],
            device_id=(g, h * 8 + low_z * 4 + y * 2 + core),
            device_id_type=MESH,
        ).start()
        return carry

    lax.fori_loop(1, line, send_a, 0)
    pltpu.make_async_copy(a_source(grp), a_all.at[own], a_recv.at[0]).start()

    def send_b(i, carry):
        t = (me + i) % count
        pltpu.make_async_remote_copy(
            src_ref=b_slabs.at[t % n_shard],
            dst_ref=b_all.at[own],
            send_sem=b_send,
            recv_sem=b_recv,
            device_id=(t // n_shard, t % n_shard),
            device_id_type=MESH,
        ).start()
        return carry

    def forward(slot, c, yy, lz, send_sem, recv_sem):
        pltpu.make_async_remote_copy(
            src_ref=a_all.at[slot],
            dst_ref=a_all.at[slot],
            send_sem=send_sem,
            recv_sem=recv_sem,
            device_id=(grp, high_z * 8 + lz * 4 + yy * 2 + c),
            device_id_type=MESH,
        ).start()

    def wait_bytes(ref, sem):
        pltpu.make_async_copy(ref, ref, sem).wait()

    def relay(i, carry):
        wait_bytes(a_all.at[0], a_recv.at[i])
        slot = slot_of(core, y, low_z, origin(i))
        forward(slot, core, y, 1 - low_z, a_send_z, a_recv_z.at[i])
        forward(slot, core, 1 - y, low_z, a_send_y, a_recv_y.at[i])
        forward(slot, 1 - core, y, low_z, a_send_c, a_recv_c)
        return carry

    def relay_z(i, carry):
        wait_bytes(a_all.at[0], a_recv_z.at[i])
        slot = slot_of(core, y, 1 - low_z, origin(i))
        forward(slot, core, 1 - y, low_z, a_send_y, a_recv_y.at[line + i])
        forward(slot, 1 - core, y, low_z, a_send_c, a_recv_c)
        return carry

    def relay_y(i, carry):
        wait_bytes(a_all.at[0], a_recv_y.at[i])
        lz = (low_z + i // line) % 2
        slot = slot_of(core, 1 - y, lz, origin(i % line))
        forward(slot, 1 - core, y, low_z, a_send_c, a_recv_c)
        return carry

    cuts = [1 + (count - 1) * k // 3 for k in range(4)]
    lax.fori_loop(0, 1, relay, 0)
    lax.fori_loop(cuts[0], cuts[1], send_b, 0)
    pltpu.make_async_copy(b_slabs.at[shard], b_all.at[own], b_recv).start()

    inputs[2].wait()
    inputs[3].wait()
    wide = rows * tok
    win = jnp.concatenate([win_ref[...]] * rows, axis=0)
    projected = dot_rows(a_rows[...], win)
    lane = lax.broadcasted_iota(jnp.int32, (rows, wide), 1)
    row = lax.broadcasted_iota(jnp.int32, (rows, wide), 0)
    small[0:1, :] = jnp.sum(jnp.where(lane // tok == row, projected, 0.0), axis=0, keepdims=True)
    lane = lax.broadcasted_iota(jnp.int32, (1, wide), 1)
    fit = jnp.zeros((1, wide), F32)
    for j in range(cand_dev):
        fit = jnp.where(lane // rank == j, fit_ref[j], fit)
    small[1:2, :] = fit

    def base_chunk(i):
        lo, size = chunks[i]
        loads[i].wait()
        base = dot_rows(weight[pl.ds(lo, size)], win)
        high = base.astype(BF16)
        rest = base - high.astype(F32)
        mid = rest.astype(BF16)
        low = rest - mid.astype(F32)
        part = lax.broadcasted_iota(jnp.int32, base.shape, 1) // tok
        terms = jnp.where(part == 0, high.astype(F32), jnp.where(part == 1, mid.astype(F32), low))
        base_ref[pl.ds(lo, size), :] = jnp.where(part < 3, terms, 0.0).astype(BF16)

    def send_small(i, carry):
        t = (me + i) % count
        pltpu.make_async_remote_copy(
            src_ref=small,
            dst_ref=small_all.at[own],
            send_sem=s_send,
            recv_sem=s_recv,
            device_id=(t // n_shard, t % n_shard),
            device_id_type=MESH,
        ).start()
        return carry

    lax.fori_loop(1, line, relay, 0)
    lax.fori_loop(cuts[1], cuts[2], send_b, 0)
    base_chunk(0)
    lax.fori_loop(0, line, relay_z, 0)
    lax.fori_loop(1, count, send_small, 0)
    pltpu.make_async_copy(small, small_all.at[own], s_recv).start()
    lax.fori_loop(cuts[2], cuts[3], send_b, 0)
    for i in range(1, len(chunks)):
        base_chunk(i)
    lax.fori_loop(0, 2 * line, relay_y, 0)

    wait_bytes(small_all, s_recv)
    wait_bytes(b_all, b_recv)
    wait_bytes(a_all.at[pl.ds(0, 4 * line)], a_recv_c)
    wait_bytes(a_all.at[pl.ds(0, line - 1)], a_send)
    wait_bytes(a_all.at[pl.ds(0, line)], a_send_z)
    wait_bytes(a_all.at[pl.ds(0, 2 * line)], a_send_y)
    wait_bytes(a_all.at[pl.ds(0, 4 * line)], a_send_c)
    wait_bytes(b_all.at[pl.ds(0, count - 1)], b_send)
    wait_bytes(small_all.at[pl.ds(0, count - 1)], s_send)


def combine_kernel(
    n_grp, n_shard, tok, rank, perturb, step_scale,
    a_ref, b_ref, small_ref, base_ref, pert_ref, upd_ref, weighted,
):
    depth = n_shard // 8
    count, rows, ff = b_ref.shape
    wide = small_ref.shape[2]
    step = pl.program_id(0)
    cand_dev = rows // rank

    @pl.when(step == 0)
    def _():
        shape = (count, rows, wide)
        pick = lax.broadcasted_iota(jnp.int32, shape, 2) == lax.broadcasted_iota(jnp.int32, shape, 1)
        fit = jnp.broadcast_to(small_ref[:, 1:2, :], shape)
        fit = jnp.sum(jnp.where(pick, fit, 0.0), axis=2, keepdims=True)
        scaled = fit * b_ref[...].astype(F32)
        weighted[...] = scaled.reshape(count * rows, ff).astype(BF16)

    width = upd_ref.shape[1]
    at = pl.ds(pl.multiple_of(step * width, width), width)
    block = a_ref[:, :, at].astype(F32).reshape(count * rows, width).astype(BF16)
    upd_ref[...] = dot_cols(weighted[...], block) * step_scale

    @pl.when(step == 0)
    def _():
        grp = lax.axis_index("grp")
        cols = pert_ref.shape[1]
        picks = [pl.ds(cyz * n_grp * depth + grp * depth, depth) for cyz in range(8)]
        k = n_shard * rows
        shape = (depth, rows, wide)
        keep = (
            lax.broadcasted_iota(jnp.int32, shape, 2) // tok
            == lax.broadcasted_iota(jnp.int32, shape, 1)
        )
        own_b = jnp.concatenate([b_ref[p].astype(F32) for p in picks], axis=0)
        own_p = jnp.concatenate(
            [
                jnp.where(keep, jnp.broadcast_to(small_ref[p, 0:1, :], shape) * perturb, 0.0)
                for p in picks
            ],
            axis=0,
        )
        own_b = own_b.reshape(k, ff).astype(BF16)
        own_p = own_p.reshape(k, wide)
        high = own_p.astype(BF16)
        low = (own_p - high.astype(F32)).astype(BF16)
        spread = (
            lax.broadcasted_iota(jnp.int32, (wide, cols), 1) % tok
            == lax.broadcasted_iota(jnp.int32, (wide, cols), 0) % tok
        ).astype(F32).astype(BF16)
        r = lax.broadcasted_iota(jnp.int32, (k, cols), 0)
        slab = r // rows
        cyz = slab // depth
        sh = (slab % depth) * 8 + (cyz % 2) * 4 + (cyz // 2 % 2) * 2 + cyz // 4
        cand = sh * cand_dev + (r % rows) // rank
        mine = cand == lax.broadcasted_iota(jnp.int32, (k, cols), 1) // tok

        def blocks(v):
            return jnp.where(mine, jnp.dot(v, spread, preferred_element_type=F32), 0.0).astype(BF16)

        total = jnp.dot(base_ref[...], spread, preferred_element_type=F32)
        total = total + dot_cols(own_b, blocks(high)) + dot_cols(own_b, blocks(low))
        pert_ref[...] = total.astype(BF16)


def local(window, weight, factor_a, factor_b, fitness):
    tok, model_width = window.shape
    cand_dev, rank, _ = factor_a.shape
    n_shard = lax.axis_size("shard")
    n_grp = lax.axis_size("grp")
    total_cands = cand_dev * n_grp * n_shard
    perturb = 0.25 / math.sqrt(model_width)
    step_scale = 0.5 / math.sqrt(total_cands)
    rows = cand_dev * rank
    ff = weight.shape[0]
    half = model_width // n_grp
    count = n_grp * n_shard
    line = n_grp * (n_shard // 8)
    wide = rows * tok

    operands = (fitness, window, factor_a, factor_b, weight)
    n_chunks = -(-ff // ROW_CHUNK)
    vmem = pl.BlockSpec(memory_space=pltpu.VMEM)
    dma = pltpu.SemaphoreType.DMA
    a_all, b_all, small_all, base = pl.pallas_call(
        functools.partial(exchange_kernel, n_grp, n_shard),
        out_shape=(
            jax.ShapeDtypeStruct((count, rows, half), BF16),
            jax.ShapeDtypeStruct((count, rows, ff), BF16),
            jax.ShapeDtypeStruct((count, 2, wide), F32),
            jax.ShapeDtypeStruct((ff, wide), BF16),
        ),
        in_specs=[pl.BlockSpec(memory_space=pltpu.HBM)] * 5,
        out_specs=(vmem, vmem, vmem, vmem),
        scratch_shapes=[
            pltpu.SMEM(fitness.shape, F32),
            pltpu.VMEM(window.shape, BF16),
            pltpu.VMEM(factor_a.shape, BF16),
            pltpu.VMEM(factor_b.shape, BF16),
            dma((4,)),
            pltpu.VMEM((rows, model_width), BF16),
            pltpu.VMEM((n_shard, rows, ff), BF16),
            pltpu.VMEM((2, wide), F32),
            pltpu.VMEM((ff, model_width), BF16),
            dma((n_chunks,)),
            dma, dma, dma, dma, dma, dma, dma, dma,
            dma((line,)), dma((line,)), dma((2 * line,)), dma,
        ],
        compiler_params=pltpu.CompilerParams(
            collective_id=0, has_side_effects=True, vmem_limit_bytes=50 * 1024 * 1024
        ),
        name="exchange",
    )(*[pltpu.with_memory_space_constraint(v, pltpu.HBM) for v in operands])

    block = min(half, 512)
    cols = n_shard * cand_dev * tok
    whole = lambda shape: pl.BlockSpec(shape, lambda i: (0,) * len(shape))
    perturbed, update = pl.pallas_call(
        functools.partial(combine_kernel, n_grp, n_shard, tok, rank, perturb, step_scale),
        out_shape=(
            jax.ShapeDtypeStruct((ff, cols), BF16),
            jax.ShapeDtypeStruct((ff, half), F32),
        ),
        grid=(half // block,),
        in_specs=[
            vmem, vmem, vmem, vmem,
        ],
        out_specs=(
            whole((ff, cols)),
            pl.BlockSpec((ff, block), lambda i: (0, i)),
        ),
        scratch_shapes=[pltpu.VMEM((count * rows, ff), BF16)],
        compiler_params=pltpu.CompilerParams(vmem_limit_bytes=40 * 1024 * 1024),
        name="combine",
    )(a_all, b_all, small_all, base)
    return perturbed, update


def solution(mesh):
    in_specs = (
        P("grp", None),
        P("shard", None),
        P(("grp", "shard"), None, None),
        P(("grp", "shard"), None, None),
        P(("grp", "shard")),
    )
    out_specs = (P("shard", "grp"), P("shard", "grp"))
    return jax.shard_map(local, mesh=mesh, in_specs=in_specs, out_specs=out_specs, check_vma=False)
```

```python
import functools
import math

import jax
import jax.numpy as jnp
from jax import lax
from jax.experimental import pallas as pl
from jax.experimental.pallas import tpu as pltpu
from jax.sharding import PartitionSpec as P

MESH = pl.DeviceIdType.MESH
F32 = jnp.float32
BF16 = jnp.bfloat16
ROW_CHUNK = 128


def dot_rows(left, right):
    return lax.dot_general(left, right, (((1,), (1,)), ((), ())), preferred_element_type=F32)


def dot_cols(left, right):
    return lax.dot_general(left, right, (((0,), (0,)), ((), ())), preferred_element_type=F32)


def exchange_kernel(
    n_grp, n_shard, fit_hbm, win_hbm, a_hbm, b_hbm, weight_ref,
    a_all, b_all, small_all, base_ref,
    fit_ref, win_ref, a_ref, b_ref, in_sem,
    a_rows, b_slabs, small, weight, w_sem, b_send, b_recv, b_send_x, b_recv_x, s_send, s_recv,
    a_send, a_send_z, a_send_y, a_send_c, a_recv, a_recv_z, a_recv_y, a_recv_c,
):
    depth = n_shard // 8
    count = n_grp * n_shard
    line = n_grp * depth
    grp = lax.axis_index("grp")
    shard = lax.axis_index("shard")
    core = shard % 2
    y = (shard // 2) % 2
    low_z = (shard // 4) % 2
    high_z = shard // 8
    me = grp * n_shard + shard
    half = a_all.shape[2]
    cand_dev, rank, _ = a_ref.shape
    rows = cand_dev * rank
    ff = weight_ref.shape[0]
    tok = win_ref.shape[0]

    def slot_of(c, yy, lz, i):
        return i // depth * n_shard + ((c * 2 + yy) * 2 + lz) * depth + i % depth

    def slot_at(s):
        return slot_of(s % 2, s // 2 % 2, s // 4 % 2, grp * depth + s // 8)

    own = slot_at(shard)

    inputs = [
        pltpu.make_async_copy(src, dst, in_sem.at[i])
        for i, (src, dst) in enumerate(
            [(a_hbm, a_ref), (b_hbm, b_ref), (win_hbm, win_ref), (fit_hbm, fit_ref)]
        )
    ]
    for load in inputs:
        load.start()

    barrier = pltpu.get_barrier_semaphore()

    def greet(i, carry):
        t = (me + i) % count
        pl.semaphore_signal(
            barrier, inc=1, device_id=(t // n_shard, t % n_shard), device_id_type=MESH
        )
        return carry

    lax.fori_loop(1, count, greet, 0)

    chunks = [(lo, min(ROW_CHUNK, ff - lo)) for lo in range(0, ff, ROW_CHUNK)]
    loads = [
        pltpu.make_async_copy(
            weight_ref.at[pl.ds(lo, size)], weight.at[pl.ds(lo, size)], w_sem.at[i]
        )
        for i, (lo, size) in enumerate(chunks)
    ]
    for load in loads:
        load.start()

    inputs[0].wait()
    a_rows[...] = jnp.concatenate(
        [a_ref[j].astype(F32) for j in range(cand_dev)], axis=0
    ).astype(BF16)
    inputs[1].wait()
    for k in range(n_shard):
        b_slabs[k] = jnp.concatenate(
            [b_ref[j, :, k * ff : (k + 1) * ff].astype(F32) for j in range(cand_dev)], axis=0
        ).astype(BF16)

    pl.semaphore_wait(barrier, count - 1)

    def origin(i):
        g = (grp + n_grp - i // depth) % n_grp
        return g * depth + (high_z + depth - i % depth) % depth

    def a_source(g):
        return a_rows.at[:, pl.ds(pl.multiple_of(g * half, half), half)]

    def send_a(i, carry):
        g = (grp + i // depth) % n_grp
        h = (high_z + i) % depth
        pltpu.make_async_remote_copy(
            src_ref=a_source(g),
            dst_ref=a_all.at[own],
            send_sem=a_send,
            recv_sem=a_recv.at[i],
            device_id=(g, h * 8 + low_z * 4 + y * 2 + core),
            device_id_type=MESH,
        ).start()
        return carry

    lax.fori_loop(1, line, send_a, 0)
    pltpu.make_async_copy(a_source(grp), a_all.at[own], a_recv.at[0]).start()

    def send_b(i, carry):
        to = (shard + i) % n_shard
        pltpu.make_async_remote_copy(
            src_ref=b_slabs.at[to],
            dst_ref=b_all.at[own],
            send_sem=b_send,
            recv_sem=b_recv.at[i],
            device_id=(grp, to),
            device_id_type=MESH,
        ).start()
        return carry

    def cross_b(src, slot):
        def one(k, carry):
            pltpu.make_async_remote_copy(
                src_ref=src,
                dst_ref=b_all.at[slot],
                send_sem=b_send_x,
                recv_sem=b_recv_x,
                device_id=((grp + k) % n_grp, shard),
                device_id_type=MESH,
            ).start()
            return carry

        lax.fori_loop(1, n_grp, one, 0)

    def relay_b(i, carry):
        wait_bytes(b_all.at[0], b_recv.at[i])
        slot = slot_at((shard + n_shard - i) % n_shard)
        cross_b(b_all.at[slot], slot)
        return carry

    def forward(slot, c, yy, lz, send_sem, recv_sem):
        pltpu.make_async_remote_copy(
            src_ref=a_all.at[slot],
            dst_ref=a_all.at[slot],
            send_sem=send_sem,
            recv_sem=recv_sem,
            device_id=(grp, high_z * 8 + lz * 4 + yy * 2 + c),
            device_id_type=MESH,
        ).start()

    def wait_bytes(ref, sem):
        pltpu.make_async_copy(ref, ref, sem).wait()

    def relay(i, carry):
        wait_bytes(a_all.at[0], a_recv.at[i])
        slot = slot_of(core, y, low_z, origin(i))
        forward(slot, core, y, 1 - low_z, a_send_z, a_recv_z.at[i])
        forward(slot, core, 1 - y, low_z, a_send_y, a_recv_y.at[i])
        forward(slot, 1 - core, y, low_z, a_send_c, a_recv_c)
        return carry

    def relay_z(i, carry):
        wait_bytes(a_all.at[0], a_recv_z.at[i])
        slot = slot_of(core, y, 1 - low_z, origin(i))
        forward(slot, core, 1 - y, low_z, a_send_y, a_recv_y.at[line + i])
        forward(slot, 1 - core, y, low_z, a_send_c, a_recv_c)
        return carry

    def relay_y(i, carry):
        wait_bytes(a_all.at[0], a_recv_y.at[i])
        lz = (low_z + i // line) % 2
        slot = slot_of(core, 1 - y, lz, origin(i % line))
        forward(slot, 1 - core, y, low_z, a_send_c, a_recv_c)
        return carry

    lax.fori_loop(0, 1, relay, 0)
    cross_b(b_slabs.at[shard], own)
    pltpu.make_async_copy(b_slabs.at[shard], b_all.at[own], b_recv.at[0]).start()
    lax.fori_loop(1, n_shard, send_b, 0)

    inputs[2].wait()
    inputs[3].wait()
    wide = rows * tok
    win = jnp.concatenate([win_ref[...]] * rows, axis=0)
    projected = dot_rows(a_rows[...], win)
    lane = lax.broadcasted_iota(jnp.int32, (rows, wide), 1)
    row = lax.broadcasted_iota(jnp.int32, (rows, wide), 0)
    small[0:1, :] = jnp.sum(jnp.where(lane // tok == row, projected, 0.0), axis=0, keepdims=True)
    lane = lax.broadcasted_iota(jnp.int32, (1, wide), 1)
    fit = jnp.zeros((1, wide), F32)
    for j in range(cand_dev):
        fit = jnp.where(lane // rank == j, fit_ref[j], fit)
    small[1:2, :] = fit

    def base_chunk(i):
        lo, size = chunks[i]
        loads[i].wait()
        base = dot_rows(weight[pl.ds(lo, size)], win)
        high = base.astype(BF16)
        rest = base - high.astype(F32)
        mid = rest.astype(BF16)
        low = rest - mid.astype(F32)
        part = lax.broadcasted_iota(jnp.int32, base.shape, 1) // tok
        terms = jnp.where(part == 0, high.astype(F32), jnp.where(part == 1, mid.astype(F32), low))
        base_ref[pl.ds(lo, size), :] = jnp.where(part < 3, terms, 0.0).astype(BF16)

    def send_small(i, carry):
        t = (me + i) % count
        pltpu.make_async_remote_copy(
            src_ref=small,
            dst_ref=small_all.at[own],
            send_sem=s_send,
            recv_sem=s_recv,
            device_id=(t // n_shard, t % n_shard),
            device_id_type=MESH,
        ).start()
        return carry

    lax.fori_loop(1, line, relay, 0)
    for i in range(0, 1):
        base_chunk(i)
    lax.fori_loop(1, n_shard // 2, relay_b, 0)
    lax.fori_loop(0, line, relay_z, 0)
    lax.fori_loop(1, count, send_small, 0)
    pltpu.make_async_copy(small, small_all.at[own], s_recv).start()
    lax.fori_loop(n_shard // 2, n_shard, relay_b, 0)
    for i in range(1, len(chunks)):
        base_chunk(i)
    lax.fori_loop(0, 2 * line, relay_y, 0)

    wait_bytes(small_all, s_recv)
    wait_bytes(b_all.at[0], b_recv.at[0])
    wait_bytes(b_all.at[pl.ds(0, count - n_shard)], b_recv_x)
    wait_bytes(b_all.at[pl.ds(0, count - n_shard)], b_send_x)
    wait_bytes(a_all.at[pl.ds(0, 4 * line)], a_recv_c)
    wait_bytes(a_all.at[pl.ds(0, line - 1)], a_send)
    wait_bytes(a_all.at[pl.ds(0, line)], a_send_z)
    wait_bytes(a_all.at[pl.ds(0, 2 * line)], a_send_y)
    wait_bytes(a_all.at[pl.ds(0, 4 * line)], a_send_c)
    wait_bytes(b_all.at[pl.ds(0, n_shard - 1)], b_send)
    wait_bytes(small_all.at[pl.ds(0, count - 1)], s_send)


def combine_kernel(
    n_grp, n_shard, tok, rank, perturb, step_scale,
    a_ref, b_ref, small_ref, base_ref, pert_ref, upd_ref, weighted,
):
    depth = n_shard // 8
    count, rows, ff = b_ref.shape
    wide = small_ref.shape[2]
    step = pl.program_id(0)
    cand_dev = rows // rank

    @pl.when(step == 0)
    def _():
        shape = (count, rows, wide)
        pick = lax.broadcasted_iota(jnp.int32, shape, 2) == lax.broadcasted_iota(jnp.int32, shape, 1)
        fit = jnp.broadcast_to(small_ref[:, 1:2, :], shape)
        fit = jnp.sum(jnp.where(pick, fit, 0.0), axis=2, keepdims=True)
        scaled = fit * b_ref[...].astype(F32)
        weighted[...] = scaled.reshape(count * rows, ff).astype(BF16)

    width = upd_ref.shape[1]
    at = pl.ds(pl.multiple_of(step * width, width), width)
    block = a_ref[:, :, at].astype(F32).reshape(count * rows, width).astype(BF16)
    upd_ref[...] = dot_cols(weighted[...], block) * step_scale

    @pl.when(step == 0)
    def _():
        grp = lax.axis_index("grp")
        cols = pert_ref.shape[1]
        mine = pl.ds(grp * n_shard, n_shard)
        k = n_shard * rows
        shape = (n_shard, rows, wide)
        keep = (
            lax.broadcasted_iota(jnp.int32, shape, 2) // tok
            == lax.broadcasted_iota(jnp.int32, shape, 1)
        )
        own_b = b_ref[mine].astype(F32)
        own_p = jnp.broadcast_to(small_ref[mine, 0:1, :], shape) * perturb
        own_p = jnp.where(keep, own_p, 0.0)
        own_b = own_b.reshape(k, ff).astype(BF16)
        own_p = own_p.reshape(k, wide)
        high = own_p.astype(BF16)
        low = (own_p - high.astype(F32)).astype(BF16)
        spread = (
            lax.broadcasted_iota(jnp.int32, (wide, cols), 1) % tok
            == lax.broadcasted_iota(jnp.int32, (wide, cols), 0) % tok
        ).astype(F32).astype(BF16)
        r = lax.broadcasted_iota(jnp.int32, (k, cols), 0)
        slab = r // rows
        cyz = slab // depth
        sh = (slab % depth) * 8 + (cyz % 2) * 4 + (cyz // 2 % 2) * 2 + cyz // 4
        cand = sh * cand_dev + (r % rows) // rank
        same = cand == lax.broadcasted_iota(jnp.int32, (k, cols), 1) // tok

        def blocks(v):
            return jnp.where(same, jnp.dot(v, spread, preferred_element_type=F32), 0.0).astype(BF16)

        total = jnp.dot(base_ref[...], spread, preferred_element_type=F32)
        total = total + dot_cols(own_b, blocks(high)) + dot_cols(own_b, blocks(low))
        pert_ref[...] = total.astype(BF16)


def local(window, weight, factor_a, factor_b, fitness):
    tok, model_width = window.shape
    cand_dev, rank, _ = factor_a.shape
    n_shard = lax.axis_size("shard")
    n_grp = lax.axis_size("grp")
    total_cands = cand_dev * n_grp * n_shard
    perturb = 0.25 / math.sqrt(model_width)
    step_scale = 0.5 / math.sqrt(total_cands)
    rows = cand_dev * rank
    ff = weight.shape[0]
    half = model_width // n_grp
    count = n_grp * n_shard
    line = n_grp * (n_shard // 8)
    wide = rows * tok

    operands = (fitness, window, factor_a, factor_b, weight)
    n_chunks = -(-ff // ROW_CHUNK)
    vmem = pl.BlockSpec(memory_space=pltpu.VMEM)
    dma = pltpu.SemaphoreType.DMA
    a_all, b_all, small_all, base = pl.pallas_call(
        functools.partial(exchange_kernel, n_grp, n_shard),
        out_shape=(
            jax.ShapeDtypeStruct((count, rows, half), BF16),
            jax.ShapeDtypeStruct((count, rows, ff), BF16),
            jax.ShapeDtypeStruct((count, 2, wide), F32),
            jax.ShapeDtypeStruct((ff, wide), BF16),
        ),
        in_specs=[pl.BlockSpec(memory_space=pltpu.HBM)] * 5,
        out_specs=(vmem, vmem, vmem, vmem),
        scratch_shapes=[
            pltpu.SMEM(fitness.shape, F32),
            pltpu.VMEM(window.shape, BF16),
            pltpu.VMEM(factor_a.shape, BF16),
            pltpu.VMEM(factor_b.shape, BF16),
            dma((4,)),
            pltpu.VMEM((rows, model_width), BF16),
            pltpu.VMEM((n_shard, rows, ff), BF16),
            pltpu.VMEM((2, wide), F32),
            pltpu.VMEM((ff, model_width), BF16),
            dma((n_chunks,)),
            dma, dma((n_shard,)), dma, dma, dma, dma, dma, dma, dma, dma,
            dma((line,)), dma((line,)), dma((2 * line,)), dma,
        ],
        compiler_params=pltpu.CompilerParams(
            collective_id=0, has_side_effects=True, vmem_limit_bytes=50 * 1024 * 1024
        ),
        name="exchange",
    )(*[pltpu.with_memory_space_constraint(v, pltpu.HBM) for v in operands])

    block = min(half, 512)
    cols = n_shard * cand_dev * tok
    whole = lambda shape: pl.BlockSpec(shape, lambda i: (0,) * len(shape))
    perturbed, update = pl.pallas_call(
        functools.partial(combine_kernel, n_grp, n_shard, tok, rank, perturb, step_scale),
        out_shape=(
            jax.ShapeDtypeStruct((ff, cols), BF16),
            jax.ShapeDtypeStruct((ff, half), F32),
        ),
        grid=(half // block,),
        in_specs=[
            vmem, vmem, vmem, vmem,
        ],
        out_specs=(
            whole((ff, cols)),
            pl.BlockSpec((ff, block), lambda i: (0, i)),
        ),
        scratch_shapes=[pltpu.VMEM((count * rows, ff), BF16)],
        compiler_params=pltpu.CompilerParams(vmem_limit_bytes=40 * 1024 * 1024),
        name="combine",
    )(a_all, b_all, small_all, base)
    return perturbed, update


def solution(mesh):
    in_specs = (
        P("grp", None),
        P("shard", None),
        P(("grp", "shard"), None, None),
        P(("grp", "shard"), None, None),
        P(("grp", "shard")),
    )
    out_specs = (P("shard", "grp"), P("shard", "grp"))
    return jax.shard_map(local, mesh=mesh, in_specs=in_specs, out_specs=out_specs, check_vma=False)
```

```python
import functools
import math

import jax
import jax.numpy as jnp
from jax import lax
from jax.experimental import pallas as pl
from jax.experimental.pallas import tpu as pltpu
from jax.sharding import PartitionSpec as P

MESH = pl.DeviceIdType.MESH
F32 = jnp.float32
BF16 = jnp.bfloat16
ROW_CHUNK = 128


def dot_rows(left, right):
    return lax.dot_general(left, right, (((1,), (1,)), ((), ())), preferred_element_type=F32)


def dot_cols(left, right):
    return lax.dot_general(left, right, (((0,), (0,)), ((), ())), preferred_element_type=F32)


def exchange_kernel(
    n_grp, n_shard, fit_hbm, win_hbm, a_hbm, b_hbm, weight_ref,
    a_all, b_all, small_all, base_ref,
    fit_ref, win_ref, a_ref, b_ref, in_sem,
    a_rows, b_slabs, small, weight, w_sem, b_send, b_recv, b_send_x, b_recv_x, s_send, s_recv,
    a_send, a_send_z, a_send_y, a_send_c, a_recv, a_recv_z, a_recv_y, a_recv_c,
):
    depth = n_shard // 8
    count = n_grp * n_shard
    line = n_grp * depth
    grp = lax.axis_index("grp")
    shard = lax.axis_index("shard")
    core = shard % 2
    y = (shard // 2) % 2
    low_z = (shard // 4) % 2
    high_z = shard // 8
    me = grp * n_shard + shard
    half = a_all.shape[2]
    cand_dev, rank, _ = a_ref.shape
    rows = cand_dev * rank
    ff = weight_ref.shape[0]
    tok = win_ref.shape[0]

    def slot_of(c, yy, lz, i):
        return i // depth * n_shard + ((c * 2 + yy) * 2 + lz) * depth + i % depth

    def slot_at(s):
        return slot_of(s % 2, s // 2 % 2, s // 4 % 2, grp * depth + s // 8)

    own = slot_at(shard)

    inputs = [
        pltpu.make_async_copy(src, dst, in_sem.at[i])
        for i, (src, dst) in enumerate(
            [(a_hbm, a_ref), (b_hbm, b_ref), (win_hbm, win_ref), (fit_hbm, fit_ref)]
        )
    ]
    for load in inputs:
        load.start()

    barrier = pltpu.get_barrier_semaphore()

    def greet(i, carry):
        t = (me + i) % count
        pl.semaphore_signal(
            barrier, inc=1, device_id=(t // n_shard, t % n_shard), device_id_type=MESH
        )
        return carry

    lax.fori_loop(1, count, greet, 0)

    chunks = [(lo, min(ROW_CHUNK, ff - lo)) for lo in range(0, ff, ROW_CHUNK)]
    loads = [
        pltpu.make_async_copy(
            weight_ref.at[pl.ds(lo, size)], weight.at[pl.ds(lo, size)], w_sem.at[i]
        )
        for i, (lo, size) in enumerate(chunks)
    ]
    for load in loads:
        load.start()

    inputs[0].wait()
    a_rows[...] = jnp.concatenate(
        [a_ref[j].astype(F32) for j in range(cand_dev)], axis=0
    ).astype(BF16)
    inputs[1].wait()
    for k in range(n_shard):
        b_slabs[k] = jnp.concatenate(
            [b_ref[j, :, k * ff : (k + 1) * ff].astype(F32) for j in range(cand_dev)], axis=0
        ).astype(BF16)

    pl.semaphore_wait(barrier, count - 1)

    def origin(i):
        g = (grp + n_grp - i // depth) % n_grp
        return g * depth + (high_z + depth - i % depth) % depth

    def a_source(g):
        return a_rows.at[:, pl.ds(pl.multiple_of(g * half, half), half)]

    def send_a(i, carry):
        g = (grp + i // depth) % n_grp
        h = (high_z + i) % depth
        pltpu.make_async_remote_copy(
            src_ref=a_source(g),
            dst_ref=a_all.at[own],
            send_sem=a_send,
            recv_sem=a_recv.at[i],
            device_id=(g, h * 8 + low_z * 4 + y * 2 + core),
            device_id_type=MESH,
        ).start()
        return carry

    lax.fori_loop(1, line, send_a, 0)
    pltpu.make_async_copy(a_source(grp), a_all.at[own], a_recv.at[0]).start()

    def send_b(i, carry):
        to = (shard + i) % n_shard
        pltpu.make_async_remote_copy(
            src_ref=b_slabs.at[to],
            dst_ref=b_all.at[own],
            send_sem=b_send,
            recv_sem=b_recv.at[i],
            device_id=(grp, to),
            device_id_type=MESH,
        ).start()
        return carry

    def cross_b(src, slot):
        def one(k, carry):
            pltpu.make_async_remote_copy(
                src_ref=src,
                dst_ref=b_all.at[slot],
                send_sem=b_send_x,
                recv_sem=b_recv_x,
                device_id=((grp + k) % n_grp, shard),
                device_id_type=MESH,
            ).start()
            return carry

        lax.fori_loop(1, n_grp, one, 0)

    def relay_b(i, carry):
        wait_bytes(b_all.at[0], b_recv.at[i])
        slot = slot_at((shard + n_shard - i) % n_shard)
        cross_b(b_all.at[slot], slot)
        return carry

    def forward(slot, c, yy, lz, send_sem, recv_sem):
        pltpu.make_async_remote_copy(
            src_ref=a_all.at[slot],
            dst_ref=a_all.at[slot],
            send_sem=send_sem,
            recv_sem=recv_sem,
            device_id=(grp, high_z * 8 + lz * 4 + yy * 2 + c),
            device_id_type=MESH,
        ).start()

    def wait_bytes(ref, sem):
        pltpu.make_async_copy(ref, ref, sem).wait()

    def relay(i, carry):
        wait_bytes(a_all.at[0], a_recv.at[i])
        slot = slot_of(core, y, low_z, origin(i))
        forward(slot, core, y, 1 - low_z, a_send_z, a_recv_z.at[i])
        forward(slot, core, 1 - y, low_z, a_send_y, a_recv_y.at[i])
        forward(slot, 1 - core, y, low_z, a_send_c, a_recv_c)
        return carry

    def relay_z(i, carry):
        wait_bytes(a_all.at[0], a_recv_z.at[i])
        slot = slot_of(core, y, 1 - low_z, origin(i))
        forward(slot, core, 1 - y, low_z, a_send_y, a_recv_y.at[line + i])
        forward(slot, 1 - core, y, low_z, a_send_c, a_recv_c)
        return carry

    def relay_y(i, carry):
        wait_bytes(a_all.at[0], a_recv_y.at[i])
        lz = (low_z + i // line) % 2
        slot = slot_of(core, 1 - y, lz, origin(i % line))
        forward(slot, 1 - core, y, low_z, a_send_c, a_recv_c)
        return carry

    lax.fori_loop(0, 1, relay, 0)
    cross_b(b_slabs.at[shard], own)
    pltpu.make_async_copy(b_slabs.at[shard], b_all.at[own], b_recv.at[0]).start()
    lax.fori_loop(1, n_shard, send_b, 0)

    inputs[2].wait()
    inputs[3].wait()
    wide = rows * tok
    win = jnp.concatenate([win_ref[...]] * rows, axis=0)
    projected = dot_rows(a_rows[...], win)
    lane = lax.broadcasted_iota(jnp.int32, (rows, wide), 1)
    row = lax.broadcasted_iota(jnp.int32, (rows, wide), 0)
    small[0:1, :] = jnp.sum(jnp.where(lane // tok == row, projected, 0.0), axis=0, keepdims=True)
    lane = lax.broadcasted_iota(jnp.int32, (1, wide), 1)
    fit = jnp.zeros((1, wide), F32)
    for j in range(cand_dev):
        fit = jnp.where(lane // rank == j, fit_ref[j], fit)
    small[1:2, :] = fit

    def base_chunk(i):
        lo, size = chunks[i]
        loads[i].wait()
        base = dot_rows(weight[pl.ds(lo, size)], win)
        high = base.astype(BF16)
        rest = base - high.astype(F32)
        mid = rest.astype(BF16)
        low = rest - mid.astype(F32)
        part = lax.broadcasted_iota(jnp.int32, base.shape, 1) // tok
        terms = jnp.where(part == 0, high.astype(F32), jnp.where(part == 1, mid.astype(F32), low))
        base_ref[pl.ds(lo, size), :] = jnp.where(part < 3, terms, 0.0).astype(BF16)

    def send_small(i, carry):
        t = (me + i) % count
        pltpu.make_async_remote_copy(
            src_ref=small,
            dst_ref=small_all.at[own],
            send_sem=s_send,
            recv_sem=s_recv,
            device_id=(t // n_shard, t % n_shard),
            device_id_type=MESH,
        ).start()
        return carry

    lax.fori_loop(1, line, relay, 0)
    for i in range(0, 1):
        base_chunk(i)
    lax.fori_loop(1, n_shard // 2, relay_b, 0)
    lax.fori_loop(0, line, relay_z, 0)
    lax.fori_loop(1, count, send_small, 0)
    pltpu.make_async_copy(small, small_all.at[own], s_recv).start()
    lax.fori_loop(n_shard // 2, n_shard, relay_b, 0)
    for i in range(1, len(chunks)):
        base_chunk(i)
    lax.fori_loop(0, 2 * line, relay_y, 0)

    wait_bytes(small_all, s_recv)
    wait_bytes(b_all.at[0], b_recv.at[0])
    wait_bytes(b_all.at[pl.ds(0, count - n_shard)], b_recv_x)
    wait_bytes(b_all.at[pl.ds(0, count - n_shard)], b_send_x)
    wait_bytes(a_all.at[pl.ds(0, 4 * line)], a_recv_c)
    wait_bytes(a_all.at[pl.ds(0, line - 1)], a_send)
    wait_bytes(a_all.at[pl.ds(0, line)], a_send_z)
    wait_bytes(a_all.at[pl.ds(0, 2 * line)], a_send_y)
    wait_bytes(a_all.at[pl.ds(0, 4 * line)], a_send_c)
    wait_bytes(b_all.at[pl.ds(0, n_shard - 1)], b_send)
    wait_bytes(small_all.at[pl.ds(0, count - 1)], s_send)


def combine_kernel(
    n_grp, n_shard, tok, rank, perturb, step_scale,
    a_ref, b_ref, small_ref, base_ref, pert_ref, upd_ref, weighted,
):
    depth = n_shard // 8
    count, rows, ff = b_ref.shape
    wide = small_ref.shape[2]
    step = pl.program_id(0)
    cand_dev = rows // rank

    @pl.when(step == 0)
    def _():
        shape = (count, rows, wide)
        pick = lax.broadcasted_iota(jnp.int32, shape, 2) == lax.broadcasted_iota(jnp.int32, shape, 1)
        fit = jnp.broadcast_to(small_ref[:, 1:2, :], shape)
        fit = jnp.sum(jnp.where(pick, fit, 0.0), axis=2, keepdims=True)
        scaled = fit * b_ref[...].astype(F32)
        weighted[...] = scaled.reshape(count * rows, ff).astype(BF16)

    width = upd_ref.shape[1]
    at = pl.ds(pl.multiple_of(step * width, width), width)
    block = a_ref[:, :, at].astype(F32).reshape(count * rows, width).astype(BF16)
    upd_ref[...] = dot_cols(weighted[...], block) * step_scale

    @pl.when(step == 0)
    def _():
        grp = lax.axis_index("grp")
        cols = pert_ref.shape[1]
        mine = pl.ds(grp * n_shard, n_shard)
        k = n_shard * rows
        shape = (n_shard, rows, wide)
        keep = (
            lax.broadcasted_iota(jnp.int32, shape, 2) // tok
            == lax.broadcasted_iota(jnp.int32, shape, 1)
        )
        own_b = b_ref[mine].astype(F32)
        own_p = jnp.broadcast_to(small_ref[mine, 0:1, :], shape) * perturb
        own_p = jnp.where(keep, own_p, 0.0)
        own_b = own_b.reshape(k, ff).astype(BF16)
        own_p = own_p.reshape(k, wide)
        high = own_p.astype(BF16)
        low = (own_p - high.astype(F32)).astype(BF16)
        spread = (
            lax.broadcasted_iota(jnp.int32, (wide, cols), 1) % tok
            == lax.broadcasted_iota(jnp.int32, (wide, cols), 0) % tok
        ).astype(F32).astype(BF16)
        r = lax.broadcasted_iota(jnp.int32, (k, cols), 0)
        slab = r // rows
        cyz = slab // depth
        sh = (slab % depth) * 8 + (cyz % 2) * 4 + (cyz // 2 % 2) * 2 + cyz // 4
        cand = sh * cand_dev + (r % rows) // rank
        same = cand == lax.broadcasted_iota(jnp.int32, (k, cols), 1) // tok

        def blocks(v):
            return jnp.where(same, jnp.dot(v, spread, preferred_element_type=F32), 0.0).astype(BF16)

        total = jnp.dot(base_ref[...], spread, preferred_element_type=F32)
        total = total + dot_cols(own_b, blocks(high)) + dot_cols(own_b, blocks(low))
        pert_ref[...] = total.astype(BF16)


def local(window, weight, factor_a, factor_b, fitness):
    tok, model_width = window.shape
    cand_dev, rank, _ = factor_a.shape
    n_shard = lax.axis_size("shard")
    n_grp = lax.axis_size("grp")
    total_cands = cand_dev * n_grp * n_shard
    perturb = 0.25 / math.sqrt(model_width)
    step_scale = 0.5 / math.sqrt(total_cands)
    rows = cand_dev * rank
    ff = weight.shape[0]
    half = model_width // n_grp
    count = n_grp * n_shard
    line = n_grp * (n_shard // 8)
    wide = rows * tok

    operands = (fitness, window, factor_a, factor_b, weight)
    n_chunks = -(-ff // ROW_CHUNK)
    vmem = pl.BlockSpec(memory_space=pltpu.VMEM)
    dma = pltpu.SemaphoreType.DMA
    a_all, b_all, small_all, base = pl.pallas_call(
        functools.partial(exchange_kernel, n_grp, n_shard),
        out_shape=(
            jax.ShapeDtypeStruct((count, rows, half), BF16),
            jax.ShapeDtypeStruct((count, rows, ff), BF16),
            jax.ShapeDtypeStruct((count, 2, wide), F32),
            jax.ShapeDtypeStruct((ff, wide), BF16),
        ),
        in_specs=[pl.BlockSpec(memory_space=pltpu.HBM)] * 5,
        out_specs=(vmem, vmem, vmem, vmem),
        scratch_shapes=[
            pltpu.SMEM(fitness.shape, F32),
            pltpu.VMEM(window.shape, BF16),
            pltpu.VMEM(factor_a.shape, BF16),
            pltpu.VMEM(factor_b.shape, BF16),
            dma((4,)),
            pltpu.VMEM((rows, model_width), BF16),
            pltpu.VMEM((n_shard, rows, ff), BF16),
            pltpu.VMEM((2, wide), F32),
            pltpu.VMEM((ff, model_width), BF16),
            dma((n_chunks,)),
            dma, dma((n_shard,)), dma, dma, dma, dma, dma, dma, dma, dma,
            dma((line,)), dma((line,)), dma((2 * line,)), dma,
        ],
        compiler_params=pltpu.CompilerParams(
            collective_id=0, has_side_effects=True, vmem_limit_bytes=50 * 1024 * 1024
        ),
        name="exchange",
    )(*[pltpu.with_memory_space_constraint(v, pltpu.HBM) for v in operands])

    block = min(half, 1024)
    cols = n_shard * cand_dev * tok
    whole = lambda shape: pl.BlockSpec(shape, lambda i: (0,) * len(shape))
    perturbed, update = pl.pallas_call(
        functools.partial(combine_kernel, n_grp, n_shard, tok, rank, perturb, step_scale),
        out_shape=(
            jax.ShapeDtypeStruct((ff, cols), BF16),
            jax.ShapeDtypeStruct((ff, half), F32),
        ),
        grid=(half // block,),
        in_specs=[
            vmem, vmem, vmem, vmem,
        ],
        out_specs=(
            whole((ff, cols)),
            pl.BlockSpec((ff, block), lambda i: (0, i)),
        ),
        scratch_shapes=[pltpu.VMEM((count * rows, ff), BF16)],
        compiler_params=pltpu.CompilerParams(vmem_limit_bytes=40 * 1024 * 1024),
        name="combine",
    )(a_all, b_all, small_all, base)
    return perturbed, update


def solution(mesh):
    in_specs = (
        P("grp", None),
        P("shard", None),
        P(("grp", "shard"), None, None),
        P(("grp", "shard"), None, None),
        P(("grp", "shard")),
    )
    out_specs = (P("shard", "grp"), P("shard", "grp"))
    return jax.shard_map(local, mesh=mesh, in_specs=in_specs, out_specs=out_specs, check_vma=False)
```
